32 devices in a mesh: dp: 4 (over z), seq: 8 (over y, x, core).
Axes of the slice: x: 2, y: 2, z: 4, core: 2. Of those that a mesh axis runs over, the one named last changes fastest.
Arguments:
- queries: bfloat16 [4096, 64, 128], P(('dp', 'seq')), parts along dimension 0, may hold values from -52 to 52
- keys: bfloat16 [4096, 8, 128], P(('dp', 'seq')), parts along dimension 0, may hold values from -6 to 6
- values: bfloat16 [4096, 8, 128], P(('dp', 'seq')), parts along dimension 0, may hold values from -6 to 6
- doc_ids: int32 [4096], P(('dp', 'seq')), parts along dimension 0, may hold values from 0 to 7, never falling along the last dimension, each value on 1 to 512 neighbouring positions
- counts: int32 [32], P('dp'), parts along dimension 0, may hold values from 64 to 128
Outputs:
- attended: bfloat16 [4096, 64, 128], P(('dp', 'seq')), parts along dimension 0
The draws below stay inside these ranges and needn't reach their ends.
There are 4 independent parts, one for each index of `dp`. The reference program is written for one: setup_inputs(seed, part) draws one part's arguments, and reference() takes and returns one part's arrays. A program takes and returns all parts, laid end to end along the dimension named above; each array names one. Nothing has to cross between parts.
Inputs may be any that keep to these rules, and one draw needn't show every extreme that they name: `doc_ids`: document numbers never fall along the sequence; each document has 1 to 512 positions. The first counts[j] positions of shard j are real tokens, the others padding.
All inputs are finite; a program needn't handle non-finite values.
Results may differ from the reference program's by a relative error of at most 0.003.
Values may be sent and summed in bfloat16 or wider, within the bound.
A program may use at most 64 MiB of HBM per device.

```python
import math
import jax
import jax.numpy as jnp
import numpy as np
from jax import lax

QUERY_HEAD_COUNT = 64
KEY_VALUE_HEADS = 8
HEAD_WIDTH = 128
S_DEV = 128
BLOCK_POSITIONS = 512
DOC_MOST = 512
SEQUENCE_LENGTH = 1024
DOCS = 8
N_SEQ = 8


def draw_pair(key):
    base = jax.random.fold_in(key, 11)
    key_query, key_random_seed = jax.random.split(base)
    query_draw = jnp.clip(jax.random.normal(key_query, (SEQUENCE_LENGTH, QUERY_HEAD_COUNT, HEAD_WIDTH), jnp.float32), -6.0, 6.0)
    key_sample = jnp.clip(jax.random.normal(key_random_seed, (SEQUENCE_LENGTH, KEY_VALUE_HEADS, HEAD_WIDTH), jnp.float32), -6.0, 6.0)
    return (query_draw, key_sample)


def draw_queries(key, part):
    return draw_pair(key)[0].astype(jnp.bfloat16)


def draw_keys(key, part):
    return draw_pair(key)[1].astype(jnp.bfloat16)


def plant(values, stream_key, low, largest):
    longest = values.shape.index(max(values.shape))
    spots = []
    for shift in (0, 1):
        where = [jax.random.randint(jax.random.fold_in(stream_key, axis), (), 0, length) for axis, length in enumerate(values.shape)]
        where[longest] = (where[longest] + shift) % values.shape[longest]
        spots.append(tuple(where))
    return values.at[spots[0]].set(low).at[spots[1]].set(largest)


def levels(rng, extent, cuts, least, top_value):
    loudness = 1.0
    for dim, blocks in cuts:
        draws = jax.random.uniform(jax.random.fold_in(jax.random.fold_in(rng, 6), dim), (blocks,), jnp.float32, least / len(cuts), top_value / len(cuts))
        loudness = loudness * jnp.repeat(jnp.exp(draws), extent[dim] // blocks).reshape((-1,) + (1,) * (len(extent) - 1 - dim))
    return loudness


def profile(amount, total, most, skew):
    portions = [(1 << 20) // math.isqrt(rank ** skew) + 1 for rank in range(2, amount + 1)]
    surplus, holding = total - most - (amount - 1), [1] * (amount - 1)
    while surplus > 0:
        movable = [i for i in range(amount - 1) if holding[i] < most]
        whole, left = sum([portions[i] for i in movable]), surplus
        for i in movable:
            extra = min(most - holding[i], max(1, left * portions[i] // whole), surplus)
            holding[i] = holding[i] + extra
            surplus = surplus - extra
    return np.array([most] + holding)


def ragged(rng, count, total, most, lean):
    if count == 2:
        one = jax.random.randint(rng, (), max(1, total - most), min(most, total - 1) + 1)
        return jnp.stack([one, total - one])
    lengths = jnp.asarray(profile(count, total, most, lean), jnp.int32)
    twos = (count - 1) // 2
    donor, taker = lengths[1:1 + 2 * twos:2], lengths[2:2 + 2 * twos:2]
    margin = jnp.minimum(donor - 1, most - taker)
    shifted = jax.random.randint(jax.random.fold_in(rng, 1), (twos,), 0, 1 << 20) % (margin + 1)
    lengths = lengths.at[1:1 + 2 * twos:2].set(donor - shifted).at[2:2 + 2 * twos:2].set(taker + shifted)
    return lengths[jax.random.permutation(jax.random.fold_in(rng, 2), count)]


def centred(key, shape, spread, reach, shards=(), held_as=jnp.bfloat16):
    values = spread * jax.random.normal(key, shape, jnp.float32)
    if shards:
        values = values * levels(key, shape, shards, -0.22, 0.18)
    return jnp.clip(values, -reach, reach).astype(held_as)


def setup_inputs(seed: int = 0, part: int = 0) -> dict:
    seeds = jax.random.split(jax.random.key(seed), 6)
    part_keys = jax.random.split(jax.random.fold_in(seeds[5], part), 6)
    return {
        "queries": draw_queries(jax.random.fold_in(jax.random.fold_in(seeds[5], part), 71), part),
        "keys": draw_keys(jax.random.fold_in(jax.random.fold_in(seeds[5], part), 71), part),
        "values": centred(part_keys[2], (SEQUENCE_LENGTH, KEY_VALUE_HEADS, HEAD_WIDTH), 1.0, 6.0, ((0, 8),)),
        "doc_ids": jnp.searchsorted(jnp.cumsum(ragged(part_keys[3], DOCS, SEQUENCE_LENGTH, DOC_MOST, 2)), jnp.arange(SEQUENCE_LENGTH), side="right").astype(jnp.int32),
        "counts": plant(jax.random.randint(part_keys[4], (N_SEQ,), S_DEV // 2, S_DEV + 1), jax.random.fold_in(part_keys[4], 1), S_DEV // 2, S_DEV).astype(jnp.int32),
    }


def reference(queries, keys, values, doc_ids, counts):
    row_count = queries.shape[0]
    shard_rows = row_count // N_SEQ
    queries_per_group = QUERY_HEAD_COUNT // KEY_VALUE_HEADS
    score_scale = 1.0 / math.sqrt(HEAD_WIDTH)
    positions = jnp.arange(row_count, dtype=jnp.int32)
    live_rows = positions % shard_rows < jnp.repeat(counts, shard_rows, total_repeat_length=row_count)
    keys_float = keys.astype(jnp.float32)
    values_float = values.astype(jnp.float32)

    def one_block(start):
        query_tile_rows = lax.dynamic_slice_in_dim(queries, start, BLOCK_POSITIONS, 0).astype(jnp.float32)
        query_tile_rows = query_tile_rows.reshape(BLOCK_POSITIONS, KEY_VALUE_HEADS, queries_per_group, HEAD_WIDTH)
        scores = jnp.einsum('qhgd,khd->hgqk', query_tile_rows, keys_float, precision=lax.Precision.HIGHEST) * score_scale
        query_pos = start + jnp.arange(BLOCK_POSITIONS, dtype=jnp.int32)
        query_doc = lax.dynamic_slice_in_dim(doc_ids, start, BLOCK_POSITIONS, 0)
        query_live = lax.dynamic_slice_in_dim(live_rows, start, BLOCK_POSITIONS, 0)
        allowed = (doc_ids[None, :] == query_doc[:, None]) & (positions[None, :] <= query_pos[:, None]) & live_rows[None, :]
        masked = jnp.where(allowed, scores, -1e+30)
        top = lax.optimization_barrier(jnp.max(masked, axis=-1, keepdims=True))
        weights = jnp.where(allowed, jnp.exp(scores - top), 0.0)
        norm_sum = lax.optimization_barrier(jnp.sum(weights, axis=-1))
        rounded = weights.astype(jnp.bfloat16).astype(jnp.float32)
        mixed = jnp.einsum('hgqk,khd->qhgd', rounded, values_float, precision=lax.Precision.HIGHEST)
        norm_rows = jnp.transpose(norm_sum, (2, 0, 1))[:, :, :, None]
        norm_rows = jnp.where(query_live[:, None, None, None], norm_rows, 1.0)
        output = jnp.where(query_live[:, None, None, None], mixed / norm_rows, 0.0)
        return output.reshape(BLOCK_POSITIONS, QUERY_HEAD_COUNT, HEAD_WIDTH).astype(jnp.bfloat16)
    starts = jnp.arange(0, row_count, BLOCK_POSITIONS, dtype=jnp.int32)
    blocks = lax.map(one_block, starts)
    return blocks.reshape(row_count, QUERY_HEAD_COUNT, HEAD_WIDTH)
```

```python
import functools
import math

import jax
import jax.numpy as jnp
from jax import lax
from jax.experimental import pallas as pl
from jax.experimental.pallas import tpu as pltpu
from jax.sharding import PartitionSpec as P

DOC_MOST = 512
MESH = pl.DeviceIdType.MESH
NEG = -1e30


def kernel(
    n, reach, tile,
    counts_ref, q_hbm, kv_hbm, doc_row_ref, doc_col_ref, out_hbm,
    win, q_vmem, o_vmem, dwin, bias,
    own_sem, q_sem, o_sem, send_sem, recv_sem, dsend_sem, drecv_sem,
):
    me = lax.axis_index("seq")
    heads, shard_rows, group, width = q_vmem.shape
    blocks = reach + 1
    keys_all = blocks * shard_rows
    rows = shard_rows * group
    tree = n == 8 and reach == 4

    def own_copy(h):
        return pltpu.make_async_copy(kv_hbm.at[h], win.at[h, :, reach], own_sem.at[h])

    def q_copy(h):
        return pltpu.make_async_copy(q_hbm.at[:, h], q_vmem.at[h], q_sem.at[h])

    def o_copy(h):
        return pltpu.make_async_copy(o_vmem.at[h], out_hbm.at[:, h], o_sem.at[h])

    def send(h, kind, from_off, to, to_off):
        return pltpu.make_async_remote_copy(
            src_ref=win.at[h, :, reach - from_off],
            dst_ref=win.at[h, :, reach - to_off],
            send_sem=send_sem.at[h, kind],
            recv_sem=recv_sem.at[h, to_off - 1],
            device_id={"seq": to},
            device_id_type=MESH,
        )

    def send_docs(off):
        return pltpu.make_async_remote_copy(
            src_ref=doc_row_ref,
            dst_ref=dwin.at[reach - off],
            send_sem=dsend_sem.at[off - 1],
            recv_sem=drecv_sem.at[off - 1],
            device_id={"seq": lax.rem(me + off, n)},
            device_id_type=MESH,
        )

    def wait_block(h, off):
        send(h, 0, 0, lax.rem(me + 1, n), off).wait_recv()

    def loop(body, count=None):
        lax.fori_loop(0, heads if count is None else count, lambda i, c: (body(i), c)[1], 0)

    loop(lambda h: own_copy(h).start())
    loop(lambda h: q_copy(h).start())

    barrier = pltpu.get_barrier_semaphore()
    for step in range(1, n):
        pl.semaphore_signal(
            barrier, inc=1, device_id={"seq": lax.rem(me + step, n)}, device_id_type=MESH
        )
    pl.semaphore_wait(barrier, n - 1)

    even = lax.rem(me, 2) == 0
    chip_odd = lax.rem(me // 2, 2) == 1
    if tree:
        own_sends = [
            (0, jnp.logical_not(chip_odd), 2),
            (1, me < 4, 4),
            (2, even, 1),
        ]
    else:
        own_sends = [(off - 1, me + off < n, off) for off in range(1, reach + 1)]

    for off in range(1, reach + 1):
        @pl.when(me + off < n)
        def _(off=off):
            send_docs(off).start()

    def start_own(h):
        own_copy(h).wait()
        for kind, cond, off in own_sends:
            @pl.when(cond)
            def _(kind=kind, off=off):
                send(h, kind, 0, lax.rem(me + off, n), off).start()

    loop(start_own)

    for off in range(1, reach + 1):
        @pl.when(me < off)
        def _(off=off):
            dwin[reach - off] = jnp.full(dwin.shape[1:], -1, jnp.int32)

            def clear(h):
                win[h, :, reach - off] = jnp.zeros((2, shard_rows, width), win.dtype)

            loop(clear)

    for off in range(1, reach + 1):
        @pl.when(me >= off)
        def _(off=off):
            send_docs(off).wait_recv()

    lane = lax.broadcasted_iota(jnp.int32, (shard_rows, shard_rows), 1)
    row = lax.broadcasted_iota(jnp.int32, (shard_rows, shard_rows), 0)
    for slot in range(blocks):
        off = reach - slot
        count = counts_ref[lax.max(me - off, 0)]
        docs = doc_row_ref[0:1, :] if off == 0 else dwin[slot, 0:1, :]
        allowed = (docs == doc_col_ref[...]) & (lane < count)
        if off == 0:
            allowed = allowed & (lane <= row)
        part = jnp.where(allowed, 0.0, NEG).astype(jnp.float32)
        part = jnp.broadcast_to(part[:, None, :], (shard_rows, group, shard_rows))
        bias[:, slot * shard_rows : (slot + 1) * shard_rows] = part.reshape(rows, shard_rows)

    own_count = counts_ref[me]
    factor = math.log2(math.e) / math.sqrt(width)

    def partner():
        return me + 1 - 2 * lax.rem(me, 2)

    def relay_two(h):
        wait_block(h, 2)

        @pl.when(even)
        def _():
            send(h, 3, 2, partner(), 3).start()

        @pl.when(jnp.logical_not(even))
        def _():
            send(h, 3, 2, partner(), 1).start()

    def stage_a(h):
        @pl.when(me >= 4)
        def _():
            wait_block(h, 4)

            @pl.when(me >= 6)
            def _():
                send(h, 5, 4, me - 2, 2).start()

            @pl.when(jnp.logical_not(even))
            def _():
                send(h, 4, 4, me - 1, 3).start()

        @pl.when(chip_odd)
        def _():
            relay_two(h)

    def is_b():
        return (me == 4) | (me == 5)

    def attend(h):
        q_copy(h).wait()
        keys = win[h, 0].reshape(keys_all, width)
        values = win[h, 1].reshape(keys_all, width)
        for start in range(0, rows, tile):
            pos = slice(start // group, (start + tile) // group)
            q = q_vmem[h, pos].reshape(tile, width)
            s = lax.dot_general(
                q, keys, (((1,), (1,)), ((), ())), preferred_element_type=jnp.float32
            )
            x = s * factor + bias[start : start + tile, :]
            top = jnp.max(x, axis=-1, keepdims=True)
            p = jnp.exp2(x - top)
            norm = jnp.sum(p, axis=-1, keepdims=True)
            o = lax.dot_general(
                p.astype(jnp.bfloat16), values, (((1,), (0,)), ((), ())),
                preferred_element_type=jnp.float32,
            )
            r = lax.broadcasted_iota(jnp.int32, (tile, width), 0) + start
            live = r < own_count * group
            o = jnp.where(live, o / norm, 0.0).astype(jnp.bfloat16)
            o_vmem[h, pos] = o.reshape(tile // group, group, width)
        o_copy(h).start()

    def step(it):
        if tree:
            @pl.when(it < heads)
            def _():
                stage_a(it)

            @pl.when((it >= 1) & (it < heads + 1) & is_b())
            def _():
                relay_two(it - 1)

            @pl.when(it >= 2)
            def _():
                for off in (1, 3):
                    @pl.when(me >= off)
                    def _(off=off):
                        wait_block(it - 2, off)
                attend(it - 2)
        else:
            for off in range(1, reach + 1):
                @pl.when(me >= off)
                def _(off=off):
                    wait_block(it, off)
            attend(it)

    loop(step, heads + 2 if tree else heads)

    def finish(h):
        o_copy(h).wait()
        for kind, cond, off in own_sends:
            @pl.when(cond)
            def _(kind=kind, off=off):
                send(h, kind, 0, lax.rem(me + off, n), off).wait_send()
        if tree:
            @pl.when(me >= 2)
            def _():
                send(h, 3, 2, partner(), 1).wait_send()

            @pl.when((me >= 4) & jnp.logical_not(even))
            def _():
                send(h, 4, 4, me - 1, 3).wait_send()

            @pl.when(me >= 6)
            def _():
                send(h, 5, 4, me - 2, 2).wait_send()

    loop(finish)
    for off in range(1, reach + 1):
        @pl.when(me + off < n)
        def _(off=off):
            send_docs(off).wait_send()


def local(n, queries, keys, values, doc_ids, counts):
    shard_rows, q_heads, width = queries.shape
    heads = keys.shape[1]
    group = q_heads // heads
    reach = min((DOC_MOST + shard_rows - 1) // shard_rows, n - 1)
    rows = shard_rows * group
    kv = jnp.stack([jnp.transpose(keys, (1, 0, 2)), jnp.transpose(values, (1, 0, 2))], axis=1)
    doc_row = jnp.broadcast_to(doc_ids[None, :], (8, shard_rows))
    doc_col = jnp.broadcast_to(doc_ids[:, None], (shard_rows, shard_rows))
    out = pl.pallas_call(
        functools.partial(kernel, n, reach, 128),
        out_shape=jax.ShapeDtypeStruct((shard_rows, heads, group, width), jnp.bfloat16),
        in_specs=[
            pl.BlockSpec(memory_space=pltpu.SMEM),
            pl.BlockSpec(memory_space=pl.ANY),
            pl.BlockSpec(memory_space=pl.ANY),
            pl.BlockSpec(memory_space=pltpu.VMEM),
            pl.BlockSpec(memory_space=pltpu.VMEM),
        ],
        out_specs=pl.BlockSpec(memory_space=pl.ANY),
        scratch_shapes=[
            pltpu.VMEM((heads, 2, reach + 1, shard_rows, width), jnp.bfloat16),
            pltpu.VMEM((heads, shard_rows, group, width), jnp.bfloat16),
            pltpu.VMEM((heads, shard_rows, group, width), jnp.bfloat16),
            pltpu.VMEM((reach, 8, shard_rows), jnp.int32),
            pltpu.VMEM((rows, (reach + 1) * shard_rows), jnp.float32),
            pltpu.SemaphoreType.DMA((heads,)),
            pltpu.SemaphoreType.DMA((heads,)),
            pltpu.SemaphoreType.DMA((heads,)),
            pltpu.SemaphoreType.DMA((heads, 6)),
            pltpu.SemaphoreType.DMA((heads, reach)),
            pltpu.SemaphoreType.DMA((reach,)),
            pltpu.SemaphoreType.DMA((reach,)),
        ],
        compiler_params=pltpu.CompilerParams(collective_id=0, has_side_effects=True),
    )(counts, queries.reshape(shard_rows, heads, group, width), kv, doc_row, doc_col)
    return out.reshape(shard_rows, q_heads, width)


def solution(mesh):
    in_specs = (
        P(("dp", "seq"), None, None),
        P(("dp", "seq"), None, None),
        P(("dp", "seq"), None, None),
        P(("dp", "seq")),
        P("dp"),
    )
    out_specs = P(("dp", "seq"), None, None)
    return jax.shard_map(
        functools.partial(local, mesh.shape["seq"]),
        mesh=mesh, in_specs=in_specs, out_specs=out_specs, check_vma=False,
    )
```

```python
import functools
import math

import jax
import jax.numpy as jnp
from jax import lax
from jax.experimental import pallas as pl
from jax.experimental.pallas import tpu as pltpu
from jax.sharding import PartitionSpec as P

DOC_MOST = 512
MESH = pl.DeviceIdType.MESH
NEG = -1e30


def kernel(
    n, reach, tile,
    counts_hbm, q_hbm, k_ref, v_ref, docs_hbm, out_ref,
    win, q_vmem, dwin, bias, counts_ref, small_sem,
    q_sem, send_sem, recv_sem, dsend_sem, drecv_sem,
):
    me = lax.axis_index("seq")
    heads, shard_rows, group, width = q_vmem.shape
    blocks = reach + 1
    keys_all = blocks * shard_rows
    rows = shard_rows * group
    tree = n == 8 and reach == 4

    def q_copy(h):
        return pltpu.make_async_copy(q_hbm.at[:, h], q_vmem.at[h], q_sem.at[h])

    def send(h, part, kind, from_off, to, to_off):
        source = (k_ref, v_ref)[part].at[h] if from_off == 0 else win.at[h, part, reach - from_off]
        return pltpu.make_async_remote_copy(
            src_ref=source,
            dst_ref=win.at[h, part, reach - to_off],
            send_sem=send_sem.at[h, part, kind],
            recv_sem=recv_sem.at[h, part, to_off - 1],
            device_id={"seq": to},
            device_id_type=MESH,
        )

    def send_docs(off):
        return pltpu.make_async_remote_copy(
            src_ref=dwin.at[reach],
            dst_ref=dwin.at[reach - off],
            send_sem=dsend_sem.at[off - 1],
            recv_sem=drecv_sem.at[off - 1],
            device_id={"seq": lax.rem(me + off, n)},
            device_id_type=MESH,
        )

    def wait_block(h, part, off):
        send(h, part, 0, 0, lax.rem(me + 1, n), off).wait_recv()

    def loop(body, count=None):
        lax.fori_loop(0, heads if count is None else count, lambda i, c: (body(i), c)[1], 0)

    doc_copy = pltpu.make_async_copy(docs_hbm, dwin.at[reach], small_sem.at[0])
    count_copy = pltpu.make_async_copy(counts_hbm, counts_ref, small_sem.at[1])
    doc_copy.start()
    count_copy.start()
    loop(lambda h: q_copy(h).start())

    barrier = pltpu.get_barrier_semaphore()
    for step in range(1, n):
        pl.semaphore_signal(
            barrier, inc=1, device_id={"seq": lax.rem(me + step, n)}, device_id_type=MESH
        )
    pl.semaphore_wait(barrier, n - 1)

    even = lax.rem(me, 2) == 0
    chip_odd = lax.rem(me // 2, 2) == 1
    if tree:
        own_sends = [
            (0, jnp.logical_not(chip_odd), 2),
            (1, me < 4, 4),
            (2, even, 1),
        ]
    else:
        own_sends = [(off - 1, me + off < n, off) for off in range(1, reach + 1)]

    def start_own(h):
        for kind, cond, off in own_sends:
            @pl.when(cond)
            def _(kind=kind, off=off):
                for part in range(2):
                    send(h, part, kind, 0, lax.rem(me + off, n), off).start()

    doc_copy.wait()
    count_copy.wait()
    for off in range(1, reach + 1):
        @pl.when(me + off < n)
        def _(off=off):
            send_docs(off).start()

    loop(start_own)

    def keep_own(h):
        win[h, 0, reach] = k_ref[h]
        win[h, 1, reach] = v_ref[h]

    loop(keep_own)

    for off in range(1, reach + 1):
        @pl.when(me < off)
        def _(off=off):
            dwin[reach - off] = jnp.full(dwin.shape[1:], -1, jnp.int32)

            def clear(h):
                win[h, :, reach - off] = jnp.zeros((2, shard_rows, width), win.dtype)

            loop(clear)

    for off in range(1, reach + 1):
        @pl.when(me >= off)
        def _(off=off):
            send_docs(off).wait_recv()

    lane = lax.broadcasted_iota(jnp.int32, (shard_rows, shard_rows), 1)
    row = lax.broadcasted_iota(jnp.int32, (shard_rows, shard_rows), 0)
    doc_col = jnp.transpose(jnp.broadcast_to(dwin[reach], (shard_rows, shard_rows)))
    for slot in range(blocks):
        off = reach - slot
        count = counts_ref[lax.max(me - off, 0)]
        docs = dwin[slot]
        allowed = (docs == doc_col) & (lane < count)
        if off == 0:
            allowed = allowed & (lane <= row)
        part = jnp.where(allowed, 0.0, NEG).astype(jnp.float32)
        part = jnp.broadcast_to(part[:, None, :], (shard_rows, group, shard_rows))
        bias[:, slot * shard_rows : (slot + 1) * shard_rows] = part.reshape(rows, shard_rows)

    own_count = counts_ref[me]
    factor = math.log2(math.e) / math.sqrt(width)

    def partner():
        return me + 1 - 2 * lax.rem(me, 2)

    def relay_two(h, part):
        wait_block(h, part, 2)

        @pl.when(even)
        def _():
            send(h, part, 3, 2, partner(), 3).start()

        @pl.when(jnp.logical_not(even))
        def _():
            send(h, part, 3, 2, partner(), 1).start()

    def relay_four(h, part):
        wait_block(h, part, 4)

        @pl.when(me >= 6)
        def _():
            send(h, part, 5, 4, me - 2, 2).start()

        @pl.when(jnp.logical_not(even))
        def _():
            send(h, part, 4, 4, me - 1, 3).start()

    def relay(h):
        for part in range(2):
            @pl.when(me >= 4)
            def _(part=part):
                relay_four(h, part)

            @pl.when(me >= 2)
            def _(part=part):
                relay_two(h, part)

    def attend(h):
        q_copy(h).wait()
        keys = win[h, 0].reshape(keys_all, width)
        values = win[h, 1].reshape(keys_all, width)

        def scores(start):
            q = q_vmem[h, start // group : (start + tile) // group].reshape(tile, width)
            return lax.dot_general(
                q, keys, (((1,), (1,)), ((), ())), preferred_element_type=jnp.float32
            )

        s_next = scores(0)
        for start in range(0, rows, tile):
            s = s_next
            if start + tile < rows:
                s_next = scores(start + tile)
            x = s * factor + bias[start : start + tile, :]
            top = jnp.max(x, axis=-1, keepdims=True)
            p = jnp.exp2(x - top)
            norm = jnp.sum(p, axis=-1, keepdims=True)
            o = lax.dot_general(
                p.astype(jnp.bfloat16), values, (((1,), (0,)), ((), ())),
                preferred_element_type=jnp.float32,
            )
            r = lax.broadcasted_iota(jnp.int32, (tile, width), 0) + start
            o = jnp.where(r < own_count * group, o / norm, 0.0).astype(jnp.bfloat16)
            out_ref[start // group : (start + tile) // group, h] = o.reshape(
                tile // group, group, width
            )

    def arrivals(h, offs):
        for off in offs:
            @pl.when(me >= off)
            def _(off=off):
                for part in range(2):
                    wait_block(h, part, off)

    def step(it):
        if tree:
            @pl.when(it < heads)
            def _():
                relay(it)

            @pl.when(it >= 1)
            def _():
                arrivals(it - 1, (1, 3))
                attend(it - 1)
        else:
            arrivals(it, range(1, reach + 1))
            attend(it)

    loop(step, heads + 1 if tree else heads)

    def finish(h):
        for part in range(2):
            for kind, cond, off in own_sends:
                @pl.when(cond)
                def _(part=part, kind=kind, off=off):
                    send(h, part, kind, 0, lax.rem(me + off, n), off).wait_send()
            if tree:
                @pl.when(me >= 2)
                def _(part=part):
                    send(h, part, 3, 2, partner(), 1).wait_send()

                @pl.when((me >= 4) & jnp.logical_not(even))
                def _(part=part):
                    send(h, part, 4, 4, me - 1, 3).wait_send()

                @pl.when(me >= 6)
                def _(part=part):
                    send(h, part, 5, 4, me - 2, 2).wait_send()

    loop(finish)
    for off in range(1, reach + 1):
        @pl.when(me + off < n)
        def _(off=off):
            send_docs(off).wait_send()


def local(n, queries, keys, values, doc_ids, counts):
    shard_rows, q_heads, width = queries.shape
    heads = keys.shape[1]
    group = q_heads // heads
    reach = min((DOC_MOST + shard_rows - 1) // shard_rows, n - 1)
    rows = shard_rows * group
    out = pl.pallas_call(
        functools.partial(kernel, n, reach, 256),
        out_shape=jax.ShapeDtypeStruct((shard_rows, heads, group, width), jnp.bfloat16),
        in_specs=[
            pl.BlockSpec(memory_space=pltpu.HBM),
            pl.BlockSpec(memory_space=pltpu.HBM),
            pl.BlockSpec(memory_space=pltpu.VMEM),
            pl.BlockSpec(memory_space=pltpu.VMEM),
            pl.BlockSpec(memory_space=pltpu.HBM),
        ],
        out_specs=pl.BlockSpec(memory_space=pltpu.VMEM),
        scratch_shapes=[
            pltpu.VMEM((heads, 2, reach + 1, shard_rows, width), jnp.bfloat16),
            pltpu.VMEM((heads, shard_rows, group, width), jnp.bfloat16),
            pltpu.VMEM((reach + 1, 1, shard_rows), jnp.int32),
            pltpu.VMEM((rows, (reach + 1) * shard_rows), jnp.float32),
            pltpu.SMEM(counts.shape, jnp.int32),
            pltpu.SemaphoreType.DMA((2,)),
            pltpu.SemaphoreType.DMA((heads,)),
            pltpu.SemaphoreType.DMA((heads, 2, 6)),
            pltpu.SemaphoreType.DMA((heads, 2, reach)),
            pltpu.SemaphoreType.DMA((reach,)),
            pltpu.SemaphoreType.DMA((reach,)),
        ],
        compiler_params=pltpu.CompilerParams(
            collective_id=0, has_side_effects=True, vmem_limit_bytes=51 << 20
        ),
    )(
        counts,
        queries.reshape(shard_rows, heads, group, width),
        jnp.transpose(keys, (1, 0, 2)),
        jnp.transpose(values, (1, 0, 2)),
        doc_ids.reshape(1, shard_rows),
    )
    return out.reshape(shard_rows, q_heads, width)


def solution(mesh):
    in_specs = (
        P(("dp", "seq"), None, None),
        P(("dp", "seq"), None, None),
        P(("dp", "seq"), None, None),
        P(("dp", "seq")),
        P("dp"),
    )
    out_specs = P(("dp", "seq"), None, None)
    return jax.shard_map(
        functools.partial(local, mesh.shape["seq"]),
        mesh=mesh, in_specs=in_specs, out_specs=out_specs, check_vma=False,
    )
```
